128 devices in a mesh: vocab: 32 (over z, x, core), tok: 4 (over y).
Axes of the slice: x: 4, y: 4, z: 4, core: 2. Of those that a mesh axis runs over, the one named last changes fastest.
Arguments:
- hidden: bfloat16 [512, 8192], P('tok'), may hold values from -40 to 40
- head: bfloat16 [8192, 126976], P('tok', 'vocab'), may hold values from -0.06629126 to 0.06629126
- teacher_probs: bfloat16 [512, 151552], P('tok', 'vocab'), may hold values from 0.0009994507 to 1
- tile_values: bfloat16 [1536, 128, 128], P('vocab'), may hold values from 0.049804688 to 1
- tile_list: int32 [1536, 2], replicated, may hold values from 0 to 991, as said below
- token_ids: int32 [512], P('tok'), may hold values from 0 to 126975
Outputs:
- token_loss: float32 [512], P('tok')
- hidden_grad: float32 [512, 8192], P('vocab', 'tok')
The draws below stay inside these ranges and needn't reach their ends.
Inputs may be any that keep to these rules, and one draw needn't show every extreme that they name: `tile_list`: column 0 is a row tile in 0 to 36, column 1 a student column tile. Of the 48 tiles of one source, at most 4 have column tiles owned by one vocab index (index c // 31), and every source gives exactly 4 to each of 8 indices.
All inputs are finite; a program needn't handle non-finite values.
Results may differ from the reference program's by a relative error of at most 0.00056.
Values may be sent and summed in bfloat16 or wider, within the bound.
A program may use at most 128 MiB of HBM per device.

```python
import math
import jax
import jax.numpy as jnp
from jax import lax

H = 8192
TILE = 128
TT_DEV = 37
SB_DEV = 31
CAP = 4
T_SIZE = 512
TV = 151552
SV = 126976
NT = 48
N_VOCAB = 32


def draw_hidden(key, part):
    base = jnp.clip(jax.random.normal(key, (T_SIZE, H), jnp.float32), -6.0, 6.0)
    return base.astype(jnp.bfloat16)


def draw_head(key, part):
    base = jax.random.normal(jax.random.fold_in(key, 11), (H, SV), jnp.float32)
    base = jnp.clip(base, -6.0, 6.0) / math.sqrt(H)
    return base.astype(jnp.bfloat16)


def draw_tile_list(key, part):
    quarter = N_VOCAB // 4
    rank_list = jnp.concatenate([jnp.repeat(jnp.arange(quarter), CAP), jnp.arange(quarter, 3 * quarter)])

    def one_source(source):
        sub_key = jax.random.fold_in(key, source)
        order = jax.random.permutation(jax.random.fold_in(sub_key, 1), N_VOCAB)
        owners = order[rank_list]
        row_tiles = jax.random.randint(jax.random.fold_in(sub_key, 2), (NT,), 0, TT_DEV)
        offsets = jax.random.randint(jax.random.fold_in(sub_key, 3), (NT,), 0, SB_DEV)
        return jnp.stack([row_tiles, owners * SB_DEV + offsets], axis=1)
    listing = jax.vmap(one_source)(jnp.arange(N_VOCAB))
    return listing.reshape(N_VOCAB * NT, 2).astype(jnp.int32)


def with_ends(drawn, rng, least, top_value):
    dims = drawn.shape
    place = [jax.random.randint(jax.random.fold_in(rng, axis), (), 0, dims[axis]) for axis in range(len(dims))]
    drawn = drawn.at[tuple(place)].set(least)
    longest = dims.index(max(dims))
    place[longest] = (place[longest] + 1) % dims[longest]
    return drawn.at[tuple(place)].set(top_value)


def block_scale(stream_key, extent, cuts, smallest, largest):
    loudness, own = 1.0, jax.random.fold_in(stream_key, 6)
    for dim, blocks in cuts:
        heights = jnp.exp(jax.random.uniform(jax.random.fold_in(own, dim), (blocks,), jnp.float32, smallest / len(cuts), largest / len(cuts)))
        loudness = loudness * jnp.repeat(heights, extent[dim] // blocks).reshape([-1 if axis == dim else 1 for axis in range(len(extent))])
    return loudness


def setup_inputs(seed: int = 0) -> dict:
    keys = jax.random.split(jax.random.key(seed), 7)
    return {
        "hidden": draw_hidden(jax.random.fold_in(keys[6], 71), 0),
        "head": draw_head(jax.random.fold_in(keys[6], 71), 0),
        "teacher_probs": jnp.clip(jnp.exp(math.log(1.0) - 6.9083047 * jax.random.uniform(keys[2], (T_SIZE, TV), jnp.float32) ** block_scale(keys[2], (T_SIZE, TV), ((0, 4), (1, 32)), -0.2, 0.2)), 0.0009994507, 1.0).astype(jnp.bfloat16),
        "tile_values": jnp.clip(jnp.exp(math.log(1.0) - 2.9996462 * jax.random.uniform(keys[3], (N_VOCAB * NT, TILE, TILE), jnp.float32) ** block_scale(keys[3], (N_VOCAB * NT, TILE, TILE), ((0, 32),), -0.2, 0.2)), 0.049804688, 1.0).astype(jnp.bfloat16),
        "tile_list": draw_tile_list(jax.random.fold_in(keys[6], 71), 0),
        "token_ids": with_ends(jax.random.randint(keys[5], (T_SIZE,), 0, SV), jax.random.fold_in(keys[5], 1), 0, SV - 1).astype(jnp.int32),
    }


hard_weight = 0.5
loss_scale = 64.0


def reference(hidden, head, teacher_probs, tile_values, tile_list, token_ids):
    logits = jnp.dot(hidden, head, preferred_element_type=jnp.float32)
    tile_count = tile_list.shape[0]

    def add_tile(running, tile_item):
        pair, values, tile_index = tile_item
        source = (tile_index // NT).astype(jnp.int32)
        row_start = ((source * TT_DEV + pair[0]) * TILE).astype(jnp.int32)
        block = lax.dynamic_slice_in_dim(teacher_probs, row_start, TILE, 1)
        product = jnp.dot(block, values, preferred_element_type=jnp.float32)
        product = lax.optimization_barrier(product.astype(jnp.bfloat16)).astype(jnp.float32)
        col_start = (pair[1] * TILE).astype(jnp.int32)
        current = lax.dynamic_slice_in_dim(running, col_start, TILE, 1)
        running = lax.dynamic_update_slice_in_dim(running, current + product, col_start, 1)
        return running, None

    mapped, _ = lax.scan(add_tile, jnp.zeros((T_SIZE, SV), jnp.float32),
                         (tile_list, tile_values, jnp.arange(tile_count, dtype=jnp.int32)))
    mass = jnp.sum(mapped, axis=1)
    row_top = jnp.max(logits, axis=1)
    shifted = jnp.exp(logits - row_top[:, None])
    exp_total = jnp.sum(shifted, axis=1)
    positive = mapped > 0
    self_term = jnp.sum(jnp.where(positive, mapped * jnp.log(jnp.where(positive, mapped, 1.0)), 0.0), axis=1)
    cross_term = jnp.sum(mapped * logits, axis=1)
    columns = jnp.arange(SV, dtype=jnp.int32)[None, :]
    is_target = columns == token_ids[:, None]
    target = jnp.sum(jnp.where(is_target, logits, 0.0), axis=1)
    log_total = jnp.log(exp_total)
    token_loss = (self_term / mass - jnp.log(mass) - cross_term / mass + row_top + log_total
                  + hard_weight * (row_top + log_total - target))
    grad = loss_scale * ((1.0 + hard_weight) * shifted / exp_total[:, None] - mapped / mass[:, None]
                         - hard_weight * is_target.astype(jnp.float32))
    grad = grad.astype(jnp.bfloat16)
    hidden_grad = lax.dot_general(grad, head, (((1,), (1,)), ((), ())), preferred_element_type=jnp.float32)
    return token_loss, hidden_grad
```

```python
import jax
import jax.numpy as jnp
from jax import lax
from jax.experimental import pallas as pl
from jax.experimental.pallas import tpu as pltpu
from jax.sharding import PartitionSpec as P

TILE = 128
CAP = 4
NV = 32
NY = 4
QMAX = 32000.0
hard_weight = 0.5
loss_scale = 64.0
MESH = pl.DeviceIdType.MESH
CHUNKS = ((0, 1024), (1024, 1024), (2048, 1024), (3072, 896))


def dev_id(v, y):
    return (v, y)


def rcopy(src, dst, ss, rs, dev):
    return pltpu.make_async_remote_copy(
        src_ref=src, dst_ref=dst, send_sem=ss, recv_sem=rs, device_id=dev, device_id_type=MESH
    )


def where_am_i():
    v = lax.axis_index("vocab")
    y = lax.axis_index("tok")
    z, x, c = v // 8, lax.rem(v // 2, 4), lax.rem(v, 2)
    return v, y, z, x, c


def vocab_of(z, x, c):
    return (lax.rem(z, 4) * 4 + lax.rem(x, 4)) * 2 + lax.rem(c, 2)


def routing(pairs, v, blocks, row_blocks):
    nt = pairs.shape[1] // NV

    def by_source(line):
        return jnp.concatenate([line[:, i * nt : (i + 1) * nt] for i in range(NV)], axis=0)

    row, col = by_source(pairs[0:1]), by_source(pairs[1:2])
    owner = jnp.floor((col.astype(jnp.float32) + 0.5) * (1.0 / blocks)).astype(jnp.int32)
    pos = lax.broadcasted_iota(jnp.int32, owner.shape, 1)
    earlier = jnp.zeros_like(owner)
    for a in range(nt):
        hit = (owner[:, a : a + 1] == owner) & (pos > a)
        earlier = earlier + jnp.where(hit, 1, 0)
    lane = lax.broadcasted_iota(jnp.int32, (128, 128), 1)
    sub = lax.broadcasted_iota(jnp.int32, (128, 128), 0)
    src_row = lax.broadcasted_iota(jnp.int32, owner.shape, 0)
    key_row = jnp.sum(jnp.where(src_row == v, owner * CAP + earlier, 0), axis=0, keepdims=True)
    key_row = jnp.concatenate([key_row, jnp.full((1, 128 - nt), -1, jnp.int32)], axis=1)
    key_col = jnp.broadcast_to(key_row.astype(jnp.float32), (128, 128)).T
    hits = key_col == lane.astype(jnp.float32)
    slot_tile = jnp.sum(jnp.where(hits, sub, 0), axis=0, keepdims=True)
    slot_used = jnp.sum(jnp.where(hits, 1, 0), axis=0, keepdims=True)
    mine = owner == v
    pieces = []
    for k in range(CAP):
        one = mine & (earlier == k)
        got = jnp.sum(jnp.where(one, col - v * blocks - blocks, 0), axis=1, keepdims=True)
        pieces.append(got + blocks)
    col_all = jnp.broadcast_to(jnp.concatenate(pieces, axis=0).astype(jnp.float32), (128, 128))
    lane_f = lane.astype(jnp.float32)

    def summing_order(col_c, first, count_of):
        col_r = col_c.T
        before = (col_r < col_c) | ((col_r == col_c) & (lane < sub))
        rank_c = jnp.sum(jnp.where(before, 1.0, 0.0), axis=1, keepdims=True)
        at = rank_c == lane_f
        order = jnp.sum(jnp.where(at, sub, 0), axis=0, keepdims=True) - first
        same_before = (col_r == col_c) & (lane < sub)
        keep_c = jnp.max(jnp.where(same_before, 1.0, 0.0), axis=1, keepdims=True)
        keep = jnp.sum(jnp.where(at, keep_c, 0.0), axis=0, keepdims=True).astype(jnp.int32)
        upto = jnp.sum(jnp.where(col_c <= lane_f, 1, 0), axis=0, keepdims=True)
        count = jnp.sum(jnp.where(col_c == lane_f, 1, 0), axis=0, keepdims=True)
        return [
            jnp.clip(order, 0, count_of - 1),
            keep,
            jnp.clip(upto - 1, 0, count_of - 1),
            jnp.where(count > 0, 1, 0),
        ]

    early = (CAP - 1) * NV
    set_a = summing_order(jnp.where(sub < early, col_all, float(blocks)), 0, early)
    set_b = summing_order(jnp.where(sub < early, float(blocks), col_all), early, NV)
    rows = jnp.sum(jnp.where(src_row == v, row, 0), axis=0, keepdims=True)
    rows = jnp.concatenate([rows, jnp.zeros((1, 128 - nt), jnp.int32)], axis=1)
    rows_c = jnp.broadcast_to(rows.astype(jnp.float32), (128, 128)).T
    slot_row = jnp.sum(jnp.where(hits, rows_c, 0.0), axis=0, keepdims=True).astype(jnp.int32)
    slot_tile = jnp.clip(slot_tile, 0, nt - 1)
    slot_row = jnp.clip(slot_row, 0, row_blocks - 1)
    return jnp.concatenate(
        [slot_tile, slot_used, slot_row, *set_a, *set_b, jnp.zeros((5, 128), jnp.int32)], axis=0
    )


def step_kernel(
    pairs, hidden, head_hbm, teacher_hbm, tiles_hbm, ids,
    loss, out,
    logits, mapped, hid, head, teacher, tiles, feat, c_out, c_in, c_last, s_buf, part, b_out, b_in,
    tab_v, tab, stat, s_out, s_in, tids, st, st_in, gall, pp, rd, zb, xb,
    ld_sem, tab_sem, t_sem, a_ss, a_rs, f_ss, f_rs, b_ss, b_rs, s_ss, s_rs, c_ss, c_rs,
    st_ss, st_rs, e_ss, e_rs, d_ss, d_rs, z_ss, z_rs, x_ss, x_rs,
):
    v, y, z, x, c = where_am_i()
    yp, ym, y2 = lax.rem(y + 1, 4), lax.rem(y + 3, 4), lax.rem(y + 2, 4)
    partner = v + 1 - 2 * c
    nh = 8
    rows_h = head.shape[0] // nh

    loads = [
        pltpu.make_async_copy(hidden, hid, ld_sem.at[0]),
        pltpu.make_async_copy(tiles_hbm, tiles, ld_sem.at[1]),
    ] + [
        pltpu.make_async_copy(
            head_hbm.at[pl.ds(i * rows_h, rows_h)], head.at[pl.ds(i * rows_h, rows_h)], ld_sem.at[2 + i]
        )
        for i in range(nh)
    ]
    def t_copy(b):
        cols = pl.ds(pl.multiple_of(b * TILE, TILE), TILE)
        return pltpu.make_async_copy(teacher_hbm.at[:, cols], teacher.at[b], t_sem.at[b])

    loads[0].start()

    @pl.loop(0, teacher.shape[0])
    def _(b):
        t_copy(b).start()

    for ld in loads[1:]:
        ld.start()

    barrier = pltpu.get_barrier_semaphore()

    def dest_of(n):
        dc, dz, dx = n // 16, lax.rem(n // 4, 4), lax.rem(n, 4)
        return vocab_of(z + dz, x + dx, c + dc)

    def src_of(n):
        dc, dz, dx = n // 16, lax.rem(n // 4, 4), lax.rem(n, 4)
        return vocab_of(z + 4 - dz, x + 4 - dx, c + 2 - dc)

    @pl.loop(1, NV)
    def _(n):
        pl.semaphore_signal(barrier, inc=1, device_id=dev_id(dest_of(n), y), device_id_type=MESH)

    for yy in (yp, ym, y2):
        pl.semaphore_signal(barrier, inc=1, device_id=dev_id(v, yy), device_id_type=MESH)

    tab_v[...] = routing(pairs[...], v, head.shape[1] // TILE, teacher.shape[0])
    tab_copy = pltpu.make_async_copy(tab_v, tab, tab_sem.at[0])
    tab_copy.start()
    pl.semaphore_wait(barrier, NV - 1 + 3)

    kf = feat.shape[2]
    loads[0].wait()

    def a_copy(i, row, n, step, target):
        cols = pl.ds(pl.multiple_of(target * kf, kf), kf)
        row = pl.multiple_of(row, 32)
        return rcopy(
            hid.at[pl.ds(row, n), cols], feat.at[step, pl.ds(row, n)], a_ss.at[i], a_rs.at[i],
            dev_id(v, target),
        )

    a_sends = [
        a_copy(0, c * 32, 32, 0, yp),
        a_copy(1, 64 + c * 32, 32, 0, ym),
        a_copy(2, c * 64, 64, 1, y2),
        a_copy(3, 64 + c * 32, 32, 2, yp),
        a_copy(4, c * 32, 32, 2, ym),
    ]
    for cp in a_sends:
        cp.start()

    spans = ((0, 32), (64, 32), (0, 64), (64, 32), (0, 32))
    steps_of = (0, 0, 1, 2, 2)

    def forward(i, cc):
        base, n = spans[i]
        rows = pl.ds(pl.multiple_of(base + cc * n, 32), n)
        ref = feat.at[steps_of[i], rows]
        return rcopy(ref, ref, f_ss.at[i], f_rs.at[i], dev_id(partner, y))

    tab_copy.wait()
    loads[1].wait()

    @pl.loop(0, teacher.shape[0])
    def _(b):
        t_copy(b).wait()

    def slot_value(s):
        used = tab[1, s].astype(jnp.float32)
        value = jnp.dot(teacher[tab[2, s]], tiles[tab[0, s]], preferred_element_type=jnp.float32)
        return (value * used).astype(jnp.bfloat16)

    def c_slot(k, source):
        return c_last.at[source] if k == CAP - 1 else c_in.at[k * NV + source]

    def c_copy(k, n):
        return rcopy(
            c_out.at[k * NV + n], c_slot(k, v), c_ss.at[k, n], c_rs.at[k, n], dev_id(dest_of(n), y),
        )

    def send_products(k):
        @pl.loop(0, NV // 4)
        def _(g):
            values = [slot_value(dest_of(g * 4 + u) * CAP + k) for u in range(4)]
            for u in range(4):
                if u:
                    c_out[k * NV + g * 4 + u] = values[u]
                    c_copy(k, g * 4 + u).start()
                else:
                    @pl.when(g == 0)
                    def _():
                        c_slot(k, v)[...] = values[0]

                    @pl.when(g > 0)
                    def _():
                        c_out[k * NV + g * 4] = values[0]
                        c_copy(k, g * 4).start()

    send_products(0)
    send_products(1)

    def b_copy(step, q, up):
        n = CHUNKS[q][1]
        side = 0 if up else 1
        return rcopy(
            b_out.at[side, step, q, :, pl.ds(0, n)], b_in.at[side, step, q, :, pl.ds(0, n)],
            b_ss.at[side, step, q], b_rs.at[side, step, q], dev_id(v, yp if up else ym),
        )

    def s_copy(step, q, up):
        side = 0 if up else 1
        return rcopy(
            s_out.at[step, q], s_in.at[side, step, q],
            s_ss.at[side, step, q], s_rs.at[side, step, q], dev_id(v, yp if up else ym),
        )

    lane_half = lax.broadcasted_iota(jnp.int32, (1, TILE), 1) < 64
    lane64 = lax.broadcasted_iota(jnp.int32, (64, TILE), 1)
    first_col = v * logits.shape[1]
    tids[...] = jnp.broadcast_to(ids[...].astype(jnp.float32), (TILE, TILE)).T.astype(jnp.int32)

    def chunk_stats(rows, c0, width, top):
        tid = tids[rows, :] - first_col - lane64
        total, target = jnp.zeros((64, TILE), jnp.float32), jnp.zeros((64, TILE), jnp.float32)
        for t in range(c0 // TILE, (c0 + width) // TILE):
            lg = logits[rows, t * TILE : (t + 1) * TILE]
            total = total + jnp.exp(lg - top)
            target = target + jnp.where(tid == t * TILE, lg, 0.0)
        mat = jnp.where(lane64 == 0, top, 0.0)
        for i, a in ((1, total), (5, target)):
            mat = jnp.where(lane64 == i, jnp.sum(a, axis=1, keepdims=True), mat)
        return mat

    own_cols = pl.ds(pl.multiple_of(y * kf, kf), kf)
    arrivals = ((0, 1), (2,), (3, 4), ())
    forwards = []
    for step in range(4):
        for i in arrivals[step]:
            a_sends[i].wait_recv()
            fw = forward(i, c)
            fw.start()
            forwards.append(fw)
        if 1 <= step <= 2:
            send_products(step + 1)
        if step == 0:
            for ld in loads[2:]:
                ld.wait()
        for i in arrivals[step]:
            forward(i, 1 - c).wait_recv()
        for q, (c0, width) in enumerate(CHUNKS):
            def lhs():
                return feat[step] if step < 3 else hid[:, own_cols]

            n_full = width // 256

            @pl.loop(0, n_full)
            def _(t):
                cols = pl.ds(pl.multiple_of(c0 + t * 256, 256), 256)
                part[:, pl.ds(pl.multiple_of(t * 256, 256), 256)] = jnp.dot(
                    lhs(), head[:, cols], preferred_element_type=jnp.float32
                )

            if width % 256:
                part[:, n_full * 256 : width] = jnp.dot(
                    lhs(), head[:, c0 + n_full * 256 : c0 + width], preferred_element_type=jnp.float32
                )
            if step > 0:
                for up in (True, False):
                    s_copy(step - 1, q, up).wait_recv()
                line = jnp.where(lane_half, s_in[0, step - 1, q, 0:1], s_in[1, step - 1, q, 0:1])
                scales = jnp.broadcast_to(line, (TILE, TILE)).T * (1.0 / QMAX)
                for up in (True, False):
                    b_copy(step - 1, q, up).wait_recv()
            tops = []
            for side in (0, 1):
                rows = slice(side * 64, side * 64 + 64)
                top = jnp.zeros((64, 128), jnp.float32)
                for t in range(width // 128):
                    cols = slice(t * 128, (t + 1) * 128)
                    val = part[rows, cols]
                    if step > 0:
                        val = val + b_in[side, step - 1, q, :, cols].astype(jnp.float32) * scales[rows]
                    if step < 3:
                        part[rows, cols] = val
                        top = jnp.maximum(top, jnp.abs(val))
                    else:
                        logits[rows, c0 + t * 128 : c0 + (t + 1) * 128] = val
                        top = jnp.maximum(top, val) if t else val
                if step == 3:
                    stat[q, rows] = chunk_stats(rows, c0, width, jnp.max(top, axis=1, keepdims=True))
                tops.append(jnp.maximum(jnp.max(top, axis=1, keepdims=True), 1e-30))
            if step < 3:
                top = jnp.broadcast_to(jnp.concatenate(tops, axis=0), (TILE, TILE))
                s_out[step, q] = top.T[0:8]
                inv = QMAX / top
                for side in (0, 1):
                    rows = slice(side * 64, side * 64 + 64)
                    for t in range(width // 128):
                        val = part[rows, t * 128 : (t + 1) * 128] * inv[rows]
                        b_out[side, step, q, :, t * 128 : (t + 1) * 128] = (
                            jnp.round(val).astype(jnp.int32).astype(jnp.int16)
                        )
                    s_copy(step, q, side == 0).start()
                    b_copy(step, q, side == 0).start()

    lane = lax.broadcasted_iota(jnp.int32, (32, TILE), 1)
    width = logits.shape[1]
    feats = head.shape[0]
    base = v * width
    nt = width // TILE

    def c_wait(k):
        @pl.loop(1, NV)
        def _(n):
            rcopy(
                c_out.at[k * NV + n], c_slot(k, src_of(n)), c_ss.at[k, n], c_rs.at[k, n],
                dev_id(dest_of(n), y),
            ).wait_recv()

    def sum_slots(source, count, at, rows):
        def add(p, total):
            total = total * tab[at + 1, p].astype(jnp.float32)
            total = total + source[tab[at, p]][rows].astype(jnp.float32)
            s_buf[p] = total
            return total

        lax.fori_loop(0, count, add, jnp.zeros((64, TILE), jnp.float32), unroll=8)

    for k in range(CAP - 1):
        c_wait(k)
    for h in range(2):
        rows = slice(h * 64, h * 64 + 64)
        sum_slots(c_in, (CAP - 1) * NV, 3, rows)
        for j in range(nt):
            mapped[rows, j * TILE : (j + 1) * TILE] = s_buf[tab[5, j]] * tab[6, j].astype(jnp.float32)
    c_wait(CAP - 1)
    for h in range(2):
        rows = slice(h * 64, h * 64 + 64)
        sum_slots(c_last, NV, 7, rows)
        zero = jnp.zeros((64, TILE), jnp.float32)
        mass, self_t, cross = zero, zero, zero
        for j in range(nt):
            cols = slice(j * TILE, (j + 1) * TILE)
            mp = mapped[rows, cols] + s_buf[tab[9, j]] * tab[10, j].astype(jnp.float32)
            mapped[rows, cols] = mp
            mass = mass + mp
            pos = mp > 0
            self_t = self_t + jnp.where(pos, mp * jnp.log(jnp.where(pos, mp, 1.0)), 0.0)
            cross = cross + mp * logits[rows, cols]
        quarters = [stat[q, rows] for q in range(len(CHUNKS))]
        tops = [a[:, 0:1] for a in quarters]
        top = jnp.maximum(jnp.maximum(tops[0], tops[1]), jnp.maximum(tops[2], tops[3]))
        mat = jnp.zeros((64, TILE), jnp.float32)
        for a, one in zip(quarters, tops):
            mat = mat + a * jnp.where(lane64 == 1, jnp.exp(one - top), 1.0)
        mat = jnp.where(lane64 == 0, top, mat)
        for i, a in ((2, mass), (3, self_t), (4, cross)):
            mat = jnp.where(lane64 == i, jnp.sum(a, axis=1, keepdims=True), mat)
        part[rows, 0:TILE] = mat
    st[...] = part[:, 0:TILE].T[0:8]
    st_in[v] = st[...]

    @pl.loop(1, NV)
    def _(n):
        rcopy(st, st_in.at[v], st_ss.at[n], st_rs.at[n], dev_id(dest_of(n), y)).start()

    @pl.loop(1, NV)
    def _(n):
        rcopy(st, st_in.at[src_of(n)], st_ss.at[n], st_rs.at[n], dev_id(dest_of(n), y)).wait_recv()

    big = st_in[0]
    for i in range(1, NV):
        big = jnp.maximum(big, st_in[i])
    row_top = big[0:1]
    acc = jnp.zeros((8, TILE), jnp.float32)
    sub8 = lax.broadcasted_iota(jnp.int32, (8, TILE), 0)
    for i in range(NV):
        one = st_in[i]
        acc = acc + one * jnp.where(sub8 == 1, jnp.exp(one[0:1] - row_top), 1.0)
    exp_total, mass, self_term, cross_term, target = (acc[i : i + 1] for i in range(1, 6))
    log_total = jnp.log(exp_total)
    loss[...] = (
        self_term / mass - jnp.log(mass) - cross_term / mass + row_top + log_total
        + hard_weight * (row_top + log_total - target)
    )
    split = 2048
    coef = jnp.concatenate(
        [row_top, (loss_scale * (1.0 + hard_weight)) / exp_total, loss_scale / mass,
         jnp.zeros((TILE - 3, TILE), jnp.float32)], axis=0
    ).T
    part[:, 0:TILE] = coef

    def e_ref(s, kind, owner):
        first, n = ((0, 32), (0, 32), (0, 16), (16, 16))[kind]
        rows = pl.ds(pl.multiple_of(owner * 32 + first, 16), n)
        if s < 3:
            return gall.at[s, rows]
        cols = slice(0, split) if s == 3 else slice(split, width)
        return gall.at[3, rows, cols]

    def e_copy(s, kind):
        ref = e_ref(s, kind, (y, y, ym, yp)[kind])
        return rcopy(ref, ref, e_ss.at[s, kind], e_rs.at[s, kind], dev_id(v, yp if kind % 2 == 0 else ym))

    def e_wait(s, kind):
        ref = e_ref(s, kind, (ym, yp, y2, y2)[kind])
        rcopy(ref, ref, e_ss.at[s, kind], e_rs.at[s, kind], dev_id(v, yp if kind % 2 == 0 else ym)).wait_recv()

    def grad_rows(s):
        j = lax.rem(s + y, 4)
        r0 = pl.multiple_of(j * 32, 32)
        rows = pl.ds(r0, 32)
        tid = tids[rows, :] - base - lane
        cf = part[rows, 0:TILE]
        top = jnp.broadcast_to(cf[:, 0:1], (32, TILE))
        ce = jnp.broadcast_to(cf[:, 1:2], (32, TILE))
        cm = jnp.broadcast_to(cf[:, 2:3], (32, TILE))
        g0 = pl.multiple_of(y * 32, 32)
        for t in range(nt):
            cols = slice(t * TILE, (t + 1) * TILE)
            val = ce * jnp.exp(logits[rows, cols] - top) - cm * mapped[rows, cols]
            val = val - jnp.where(tid == t * TILE, loss_scale * hard_weight, 0.0)
            gall[s, pl.ds(g0, 32), cols] = val.astype(jnp.bfloat16)

    def own_out(s):
        e_copy(s, 0).start()
        e_copy(s, 1).start()

    for s in range(4):
        grad_rows(s)
        if s < 2:
            own_out(s)


    hf = feats // 2

    def d_copy(s, h):
        return rcopy(pp.at[s, h, 1 - c], rd.at[s, h], d_ss.at[s, h], d_rs.at[s, h], dev_id(partner, y))

    def one_copy(s, h, d):
        if h == 0:
            zt = lax.rem(z + d, 4)
            slot, to = zt, vocab_of(zt, x, c)
        else:
            xt = lax.rem(x + d, 4)
            slot, to = lax.rem(xt + 4 - s, 4), vocab_of(z, xt, c)
        return rcopy(pp.at[s, h, c, slot], zb.at[s, h, d - 1], z_ss.at[s, h, d - 1], z_rs.at[s, h, d - 1], dev_id(to, y))

    def one_phase(s, h):
        d_copy(s, h).wait_recv()
        for i in range(4):
            pp[s, h, c, i] = pp[s, h, c, i] + rd[s, h, i]
        for d in (2, 1, 3):
            one_copy(s, h, d).start()

    def own_slot(s, h):
        return z if h == 0 else lax.rem(x + 4 - s, 4)

    def two_dist(s, h):
        return lax.rem(s + z + 4 - x, 4) if h == 0 else lax.rem(x + 8 - s - z, 4)

    def two_copy(s, h, d):
        to = vocab_of(z, x + d, c) if h == 0 else vocab_of(z + d, x, c)
        return rcopy(pp.at[s, h, c, own_slot(s, h)], xb.at[h, d - 1], x_ss.at[s, h], x_rs.at[h, d - 1], dev_id(to, y))

    def two_phase(s, h):
        for d in (1, 2, 3):
            one_copy(s, h, d).wait_recv()
        own = own_slot(s, h)
        pp[s, h, c, own] = (pp[s, h, c, own] + zb[s, h, 0]) + (zb[s, h, 1] + zb[s, h, 2])
        for d in (1, 2, 3):
            @pl.when(two_dist(s, h) == d)
            def _():
                two_copy(s, h, d).start()

    def pass_on(s):
        e_wait(s, 0)
        e_copy(s, 2).start()
        e_wait(s, 1)
        e_copy(s, 3).start()

    def product(s, half, k0, k1, more=False):
        @pl.loop(0, hf // 512)
        def _(f):
            res = lax.dot_general(
                gall[s, :, k0:k1], head[pl.ds(pl.multiple_of(half * hf + f * 512, 512), 512), k0:k1],
                (((1,), (1,)), ((), ())), preferred_element_type=jnp.float32,
            )
            fr = pl.ds(pl.multiple_of(f * 512, 512), 512)
            for o in range(4):
                for h in range(2):
                    a = o * 32 + h * 16
                    value = res[a : a + 16]
                    if more:
                        value = value + pp[s, half, h, o, :, fr]
                    pp[s, half, h, o, :, fr] = value

    pass_on(0)
    own_out(2)
    for s in range(3):
        pass_on(s + 1)
        if s == 0:
            own_out(3)
        if s == 1:
            own_out(4)
        if s >= 1:
            one_phase(s - 1, 0)
            one_phase(s - 1, 1)
        if s >= 2:
            two_phase(s - 2, 0)
            two_phase(s - 2, 1)
        e_wait(s, 2)
        e_wait(s, 3)
        product(s, 0, 0, width)
        d_copy(s, 0).start()
        if s == 2:
            pass_on(4)
        product(s, 1, 0, width)
        d_copy(s, 1).start()
    for kind in (2, 3):
        e_wait(3, kind)
    product(3, 0, 0, split)
    one_phase(2, 0)
    one_phase(2, 1)
    two_phase(1, 0)
    two_phase(1, 1)
    product(3, 1, 0, split)
    for kind in (2, 3):
        e_wait(4, kind)
    product(3, 0, split, width, True)
    d_copy(3, 0).start()
    product(3, 1, split, width, True)
    d_copy(3, 1).start()
    one_phase(3, 0)
    one_phase(3, 1)
    two_phase(2, 0)
    two_phase(2, 1)
    two_phase(3, 0)
    two_phase(3, 1)
    own_last = (z, z)
    for h in range(2):
        for d in (1, 2, 3):
            two_copy(0, h, d).wait_recv()
        mine = pp[lax.rem(x + 4 - z, 4), h, c, own_last[h]]
        out[:, h * hf : (h + 1) * hf] = (mine + xb[h, 0]) + (xb[h, 1] + xb[h, 2])

    for s in range(5):
        for kind in range(4):
            e_copy(s, kind).wait_send()
    for s in range(4):
        for h in range(2):
            d_copy(s, h).wait_send()
            for d in (1, 2, 3):
                one_copy(s, h, d).wait_send()
            for d in (1, 2, 3):
                @pl.when(two_dist(s, h) == d)
                def _():
                    two_copy(s, h, d).wait_send()

    @pl.loop(1, NV)
    def _(n):
        rcopy(st, st_in.at[v], st_ss.at[n], st_rs.at[n], dev_id(dest_of(n), y)).wait_send()

    for cp in a_sends + forwards:
        cp.wait_send()
    for step in range(3):
        for q in range(4):
            for up in (True, False):
                b_copy(step, q, up).wait_send()
                s_copy(step, q, up).wait_send()

    for k in range(CAP):
        @pl.loop(1, NV)
        def _(n):
            c_copy(k, n).wait_send()


def any_spec():
    return pl.BlockSpec(memory_space=pl.ANY)


def vmem_spec():
    return pl.BlockSpec(memory_space=pltpu.VMEM)


def on_device(hidden, head, teacher_probs, tile_values, tile_list, token_ids):
    tok, width = hidden.shape[0], head.shape[1]
    feats, nt = head.shape[0], tile_values.shape[0]
    dma = pltpu.SemaphoreType.DMA
    f32, bf16, i16 = jnp.float32, jnp.bfloat16, jnp.int16
    loss, out = pl.pallas_call(
        step_kernel,
        out_shape=(jax.ShapeDtypeStruct((1, tok), f32), jax.ShapeDtypeStruct((16, feats), f32)),
        in_specs=[vmem_spec()] + [any_spec()] * 4 + [vmem_spec()],
        out_specs=(vmem_spec(),) * 2,
        scratch_shapes=[
            pltpu.VMEM((tok, width), f32),
            pltpu.VMEM((tok, width), f32),
            pltpu.VMEM(hidden.shape, bf16),
            pltpu.VMEM(head.shape, bf16),
            pltpu.VMEM((teacher_probs.shape[1] // TILE, tok, TILE), bf16),
            pltpu.VMEM(tile_values.shape, bf16),
            pltpu.VMEM((3, tok, feats), bf16),
            pltpu.VMEM((NV * CAP, tok, TILE), bf16),
            pltpu.VMEM((NV * (CAP - 1), tok, TILE), bf16),
            pltpu.VMEM((NV, tok, TILE), bf16),
            pltpu.VMEM((NV * (CAP - 1), 64, TILE), f32),
            pltpu.VMEM((tok, 1024), f32),
            pltpu.VMEM((2, 3, 4, 64, 1024), i16),
            pltpu.VMEM((2, 3, 4, 64, 1024), i16),
            pltpu.VMEM((16, TILE), jnp.int32),
            pltpu.SMEM((16, TILE), jnp.int32),
            pltpu.VMEM((len(CHUNKS), tok, TILE), f32),
            pltpu.VMEM((3, 4, 8, TILE), f32),
            pltpu.VMEM((2, 3, 4, 8, TILE), f32),
            pltpu.VMEM((TILE, TILE), jnp.int32),
            pltpu.VMEM((8, TILE), f32),
            pltpu.VMEM((NV, 8, TILE), f32),
            pltpu.VMEM((4, tok, width), bf16),
            pltpu.VMEM((4, 2, 2, 4, 16, feats // 2), f32),
            pltpu.VMEM((4, 2, 4, 16, feats // 2), f32),
            pltpu.VMEM((4, 2, 3, 16, feats // 2), f32),
            pltpu.VMEM((2, 3, 16, feats // 2), f32),
            dma((10,)), dma((1,)), dma((teacher_probs.shape[1] // TILE,)), dma((5,)), dma((5,)), dma((5,)), dma((5,)),
            dma((2, 3, 4)), dma((2, 3, 4)), dma((2, 3, 4)), dma((2, 3, 4)), dma((CAP, NV)), dma((CAP, NV)),
            dma((NV,)), dma((NV,)), dma((5, 4)), dma((5, 4)), dma((4, 2)), dma((4, 2)),
            dma((4, 2, 3)), dma((4, 2, 3)), dma((4, 2)), dma((2, 3)),
        ],
        compiler_params=pltpu.CompilerParams(
            collective_id=0, has_side_effects=True, vmem_limit_bytes=67043328
        ),
        name="step",
    )(tile_list.T, hidden, head, teacher_probs, tile_values, token_ids.reshape(1, tok))
    return loss.reshape(tok), out


def solution(mesh):
    in_specs = (
        P("tok", None), P("tok", "vocab"), P("tok", "vocab"), P("vocab", None, None), P(), P("tok"),
    )
    out_specs = (P("tok"), P("vocab", "tok"))
    return jax.shard_map(on_device, mesh=mesh, in_specs=in_specs, out_specs=out_specs, check_vma=False)
```
